128 devices in a mesh: seq: 16 (over z, x), tp: 8 (over y, core).
Axes of the slice: x: 4, y: 4, z: 4, core: 2. Of those that a mesh axis runs over, the one named last changes fastest.
Arguments:
- inner_x: bfloat16 [8192, 5120], P('seq', 'tp'), may hold values from -6 to 6
- gate_z: bfloat16 [8192, 5120], P('seq', 'tp'), may hold values from -6 to 6
- proj_bc: bfloat16 [8192, 256], P('seq'), may hold values from -6 to 6
- dt_raw: bfloat16 [8192, 80], P('seq', 'tp'), may hold values from -6 to 10
- a_log: float32 [80], P('tp'), may hold values from -12 to 0
- dt_bias: float32 [80], P('tp'), may hold values from -4 to -2
- d_skip: float32 [80], P('tp'), may hold values from 0.5 to 1.5
- conv_x: float32 [4, 5120], P(None, 'tp'), may hold values from -3 to 3
- bias_x: float32 [5120], P('tp'), may hold values from -3 to 3
- conv_bc: float32 [4, 256], replicated, may hold values from -3 to 3
- bias_bc: float32 [256], replicated, may hold values from -3 to 3
- norm_gain: float32 [5120], P('tp'), may hold values from 0.5 to 1.5
- w_out: bfloat16 [5120, 2560], P('tp', 'seq'), may hold values from -0.078125 to 0.078125
- d_out: bfloat16 [8192, 2560], P('seq', 'tp'), may hold values from -6 to 6
Outputs:
- output: bfloat16 [8192, 2560], P('seq', 'tp')
- grad_x: float32 [8192, 5120], P('seq', 'tp')
- grad_z: float32 [8192, 5120], P('seq', 'tp')
- grad_bc: float32 [8192, 256], P('seq')
- grad_dt: float32 [8192, 80], P('seq', 'tp')
- grad_w: float32 [5120, 2560], P('tp', 'seq')
The draws below stay inside these ranges and needn't reach their ends.
All inputs are finite; a program needn't handle non-finite values.
Results may differ from the reference program's by a relative error of at most 0.013.
Values may be sent and summed in bfloat16 or wider, within the bound.
No kernel may reach another device: no remote copies, remote signals or barrier semaphores. Data moves between devices by JAX's collectives and lax.ppermute only.
A program may use at most 192 MiB of HBM per device.

```python
import jax
import jax.numpy as jnp
from jax import lax

D = 2560
HEADS = 80
STATE = 128
KERNEL = 4
BLOCK = 256
INNER = 5120
STREAM_LENGTH = 8192
N_TP = 8


def draw_a_log(key, part):
    key_order, key_slow, key_fast = jax.random.split(jax.random.fold_in(key, 11), 3)
    ranking = jax.random.permutation(key_order, HEADS)
    keeping = ranking >= HEADS // 2
    slow_log = jnp.log(2.0 / STREAM_LENGTH) + jax.random.uniform(key_slow, (HEADS,), jnp.float32) * jnp.log(10.0)
    fast_log = jnp.log(0.3) + jax.random.uniform(key_fast, (HEADS,), jnp.float32) * jnp.log(3.0)
    return jnp.where(keeping, slow_log, fast_log).astype(jnp.float32)


def draw_dt_raw(key, part):
    key_ground, key_spots, key_raise = jax.random.split(jax.random.fold_in(key, 23), 3)
    expected_answer = jnp.clip(jax.random.normal(key_ground, (STREAM_LENGTH, HEADS), jnp.float32), -6.0, 6.0)
    marker_indices = jax.random.randint(key_spots, (8,), 0, STREAM_LENGTH)
    cluster_batches = jnp.any(jnp.arange(STREAM_LENGTH)[:, None] == marker_indices[None, :], axis=1)
    elevated_entries = jax.random.uniform(key_raise, (HEADS,), jnp.float32, 2.0, 4.0)
    return (expected_answer + jnp.where(cluster_batches[:, None], elevated_entries[None, :], 0.0)).astype(jnp.bfloat16)


def strengthened(values, own_key, source, target, blocks, factor):
    owner, partner = [(jnp.arange(values.shape[axis_at]) // (values.shape[axis_at] // blocks)).reshape([-1 if axis == axis_at else 1 for axis in range(values.ndim)]) for axis_at in (source, target)]
    chosen = jax.random.permutation(own_key, blocks)[partner]
    strong = (owner == chosen) | (owner == (partner + blocks // 2) % blocks)
    return jnp.where(strong, factor * values, values)


def shard_levels(stream_key, shape, cuts, least, largest):
    def one(position, shards_of):
        heights = jax.random.uniform(jax.random.fold_in(jax.random.fold_in(stream_key, 6), position), (shards_of,), jnp.float32, least / len(cuts), largest / len(cuts))
        return jnp.repeat(jnp.exp(heights), shape[position] // shards_of).reshape((-1,) + (1,) * (len(shape) - position - 1))

    loudness = one(*cuts[0])
    for cut in cuts[1:]:
        loudness = loudness * one(*cut)
    return loudness


def normal_values(key, extent, deviation, bound, cuts=(), kind=jnp.bfloat16):
    array = jax.random.normal(key, extent, jnp.float32) * deviation
    if len(cuts) > 0:
        array = shard_levels(key, extent, cuts, -0.22, 0.18) * array
    return jnp.clip(array, min=-bound, max=bound).astype(kind)


def heavy_noise(stream_key, dims, scale, most, cuts, heavy, kind=jnp.bfloat16):
    result = scale * jax.random.normal(stream_key, dims, jnp.float32)
    if cuts:
        result = result * shard_levels(stream_key, dims, cuts, -0.22, 0.18)
    return jnp.clip(strengthened(result, jax.random.fold_in(stream_key, 3), *heavy), -most, most).astype(kind)


def setup_inputs(seed: int = 0) -> dict:
    key_of = jax.random.split(jax.random.key(seed), 15)
    return {
        "inner_x": normal_values(key_of[0], (STREAM_LENGTH, INNER), 1.0, 6.0, ((0, 16), (1, 8))),
        "gate_z": normal_values(key_of[1], (STREAM_LENGTH, INNER), 1.0, 6.0, ((0, 16), (1, 8))),
        "proj_bc": normal_values(key_of[2], (STREAM_LENGTH, 2 * STATE), 1.0, 6.0, ((0, 16),)),
        "dt_raw": draw_dt_raw(jax.random.fold_in(key_of[14], 71), 0),
        "a_log": draw_a_log(jax.random.fold_in(key_of[14], 71), 0),
        "dt_bias": jnp.clip(-4.0 + 2.0 * jax.random.uniform(key_of[5], (HEADS,), jnp.float32) ** shard_levels(key_of[5], (HEADS,), ((0, 8),), -0.2, 0.2), -4.0, -2.0),
        "d_skip": jnp.clip(0.5 + 1.0 * jax.random.uniform(key_of[6], (HEADS,), jnp.float32) ** shard_levels(key_of[6], (HEADS,), ((0, 8),), -0.2, 0.2), 0.5, 1.5),
        "conv_x": normal_values(key_of[7], (KERNEL, INNER), KERNEL ** -0.5, 3.0, ((1, 8),), jnp.float32),
        "bias_x": normal_values(key_of[8], (INNER,), 0.5, 3.0, ((0, 8),), jnp.float32),
        "conv_bc": normal_values(key_of[9], (KERNEL, 2 * STATE), KERNEL ** -0.5, 3.0, (), jnp.float32),
        "bias_bc": normal_values(key_of[10], (2 * STATE,), 0.5, 3.0, (), jnp.float32),
        "norm_gain": jnp.clip(1.0 + 0.1 * jax.random.normal(key_of[11], (INNER,), jnp.float32), 0.5, 1.5),
        "w_out": normal_values(key_of[12], (INNER, D), INNER ** -0.5, 0.078125, ((0, 8), (1, 16))),
        "d_out": heavy_noise(key_of[13], (STREAM_LENGTH, D), 1.0, 6.0, ((0, 16), (1, 8)), (0, 1, 16, 2.0)),
    }


HIGH = lax.Precision.HIGHEST
EPSILON = 1e-05

def causal_conv(padded, weights, biases):
    kernel_taps = weights.shape[0]
    out_rows = padded.shape[0] - kernel_taps + 1
    summed = jnp.zeros((out_rows, padded.shape[1]), jnp.float32) + biases[None, :]
    for offset in range(kernel_taps):
        summed = summed + weights[offset][None, :] * padded[offset:offset + out_rows]
    return jax.nn.silu(summed)

def ssd_local(values, projected, raw_steps, a_log, dt_bias, d_skip, block, saving):
    row_count, channels = values.shape
    head_count = a_log.shape[0]
    head_size = channels // head_count
    state_size = projected.shape[1] // 2
    step_sizes = jax.nn.softplus(raw_steps + dt_bias[None, :])
    decay_logarithm = -step_sizes * jnp.exp(a_log)[None, :]
    shaped = values.reshape(row_count, head_count, head_size)
    scaled = shaped * step_sizes[:, :, None]
    block_count = row_count // block
    causal_mask = (jnp.arange(block)[:, None] >= jnp.arange(block)[None, :])[:, :, None]

    def one_block(carried_state, pieces):
        own_values, own_scaled, own_decay, own_proj = pieces
        input_map = own_proj[:, :state_size]
        output_map = own_proj[:, state_size:]
        running = jnp.cumsum(own_decay, axis=0)
        scores = jnp.dot(output_map, input_map.T, precision=HIGH)
        spread = running[:, None, :] - running[None, :, :]
        weights = jnp.exp(jnp.where(causal_mask, spread, -jnp.inf)) * scores[:, :, None]
        within = jnp.einsum('tsh,shp->thp', weights, own_scaled, precision=HIGH)
        reads = jnp.einsum('tn,hpn->thp', output_map, carried_state, precision=HIGH)
        from_state = jnp.exp(running)[:, :, None] * reads
        to_end = jnp.exp(running[-1][None, :] - running)
        fresh = jnp.einsum('shp,sn->hpn', to_end[:, :, None] * own_scaled, input_map, precision=HIGH)
        next_state = jnp.exp(running[-1])[:, None, None] * carried_state + fresh
        block_out = within + from_state + d_skip[None, :, None] * own_values
        return (next_state, block_out)
    step_fn = jax.checkpoint(one_block) if saving else one_block
    pieces = (shaped.reshape(block_count, block, head_count, head_size), scaled.reshape(block_count, block, head_count, head_size), decay_logarithm.reshape(block_count, block, head_count), projected.reshape(block_count, block, 2 * state_size))
    initial = jnp.zeros((head_count, head_size, state_size), jnp.float32)
    final_state, outputs = lax.scan(step_fn, initial, pieces)
    return (outputs.reshape(row_count, channels), final_state, lax.optimization_barrier(jnp.sum(decay_logarithm, axis=0)))

def reference(inner_x, gate_z, proj_bc, dt_raw, a_log, dt_bias, d_skip, conv_x, bias_x, conv_bc, bias_bc, norm_gain, w_out, d_out):
    kernel_taps = conv_x.shape[0]

    def region(values, projected, raw_steps):
        pad_values = jnp.concatenate([jnp.zeros((kernel_taps - 1, values.shape[1]), jnp.float32), values], 0)
        pad_proj = jnp.concatenate([jnp.zeros((kernel_taps - 1, projected.shape[1]), jnp.float32), projected], 0)
        conv_values = causal_conv(pad_values, conv_x, bias_x)
        conv_proj = causal_conv(pad_proj, conv_bc, bias_bc)
        mixed_out, final_state, decay_total = ssd_local(conv_values, conv_proj, raw_steps, a_log, dt_bias, d_skip, BLOCK, True)
        return mixed_out
    mixed_out, region_pull = jax.vjp(region, inner_x.astype(jnp.float32), proj_bc.astype(jnp.float32), dt_raw.astype(jnp.float32))
    gate_value = gate_z.astype(jnp.float32)
    gate_sigma = jax.nn.sigmoid(gate_value)
    gate_silu = jax.nn.silu(gate_value)
    gated_out = mixed_out * gate_silu
    inv_rms = lax.rsqrt(lax.optimization_barrier(jnp.sum(gated_out * gated_out, axis=1)) / INNER + EPSILON)
    normed = (gated_out * inv_rms[:, None] * norm_gain[None, :]).astype(jnp.bfloat16)
    group_size = INNER // N_TP

    def add_group(running_sum, group_index):
        normed_part = lax.dynamic_slice_in_dim(normed, group_index * group_size, group_size, 1)
        weight_part = lax.dynamic_slice_in_dim(w_out, group_index * group_size, group_size, 0)
        term = jnp.dot(normed_part, weight_part, preferred_element_type=jnp.float32)
        quantized_copy = lax.optimization_barrier(term.astype(jnp.bfloat16))
        return (running_sum + quantized_copy.astype(jnp.float32), None)
    summed, discarded_item = lax.scan(add_group, jnp.zeros((STREAM_LENGTH, D), jnp.float32), jnp.arange(N_TP, dtype=jnp.int32))
    output = summed.astype(jnp.bfloat16)
    grad_normed = lax.dot_general(d_out, w_out, (((1,), (1,)), ((), ())), preferred_element_type=jnp.float32)
    grad_w = lax.dot_general(normed, d_out, (((0,), (0,)), ((), ())), preferred_element_type=jnp.float32)
    scaled_grad = grad_normed * norm_gain[None, :]
    inner_sum = lax.optimization_barrier(jnp.sum(scaled_grad * gated_out, axis=1))
    grad_gated = inv_rms[:, None] * scaled_grad - gated_out * (inv_rms ** 3 * inner_sum / INNER)[:, None]
    grad_z = grad_gated * mixed_out * gate_sigma * (1.0 + gate_value * (1.0 - gate_sigma))
    grad_mixed = grad_gated * gate_silu
    grad_values, grad_proj, grad_steps = region_pull(grad_mixed)
    return (output, grad_values, grad_z, grad_proj, grad_steps, grad_w)
```

```python
import jax
import jax.numpy as jnp
from jax import lax
from jax.experimental import pallas as pl
from jax.experimental.pallas import tpu as pltpu
from jax.sharding import Mesh
from jax.sharding import PartitionSpec as P


SEQ = ("seq_0", "seq_1")
EPSILON = 1e-05
HEAD = 64
LANES = 128
CHUNK = 128
NEG = -1e30
F32 = jnp.float32
BF16 = jnp.bfloat16
HIGH = lax.Precision.HIGHEST


def dot(a, b, ca=1, cb=0):
    return lax.dot_general(a, b, (((ca,), (cb,)), ((), ())), preferred_element_type=F32)


def dot3(a, b, ca=1, cb=0):
    ah, al = split_two(a)
    bh, bl = split_two(b)
    return dot(ah, bh, ca, cb) + dot(al, bh, ca, cb) + dot(ah, bl, ca, cb)


def split_two(a):
    high = a.astype(BF16)
    return high, (a - high.astype(F32)).astype(BF16)


def head_map(channels):
    row = lax.broadcasted_iota(jnp.int32, (LANES, channels), 0)
    col = lax.broadcasted_iota(jnp.int32, (LANES, channels), 1)
    return jnp.where(lax.shift_right_logical(col, 6) == row, 1.0, 0.0).astype(BF16)


def per_channel(a, heads):
    high, low = split_two(a)
    return dot(high, heads) + dot(low, heads)


def per_head(a, heads):
    high, low = split_two(a)
    return dot(high, heads, 1, 1) + dot(low, heads, 1, 1)


def sigmoid(v):
    return 1.0 / (1.0 + jnp.exp(-v))


def softplus(v):
    return jnp.maximum(v, 0.0) + jnp.log1p(jnp.exp(-jnp.abs(v)))


def lower(size):
    return lax.broadcasted_iota(jnp.int32, (size, size), 0) >= lax.broadcasted_iota(
        jnp.int32, (size, size), 1
    )


def offsets(run, tokens):
    before = [jnp.zeros((1, LANES), F32)]
    for c in range(tokens // CHUNK):
        before.append(before[-1] + run[(c + 1) * CHUNK - 1 : (c + 1) * CHUNK, :])
    return before


def shard_running(run, tokens):
    before = offsets(run, tokens)
    parts = [run[c * CHUNK : (c + 1) * CHUNK, :] + before[c] for c in range(tokens // CHUNK)]
    return jnp.concatenate(parts, 0), before


def lanes_of(first):
    lane = lax.broadcasted_iota(jnp.int32, (CHUNK, LANES), 1)
    return lane < HEAD if first else lane >= HEAD


def stacked(block):
    zero = jnp.zeros_like(block)
    return jnp.concatenate(
        [jnp.where(lanes_of(True), block, zero), jnp.where(lanes_of(False), block, zero)], 0
    )


def pair_weights(run, run_t, c, pair):
    rows = slice(c * CHUNK, (c + 1) * CHUNK)
    sides = []
    for h in (2 * pair, 2 * pair + 1):
        spread = run[rows, h : h + 1] - run_t[h : h + 1, rows]
        sides.append(jnp.exp(jnp.where(lower(CHUNK), spread, NEG)))
    return jnp.concatenate(sides, 1)


def conv_body(x_ref, bc_ref, halo_ref, dt_ref, par_ref, cx_ref, bx_ref, cb_ref, bb_ref,
              xv_ref, dx_ref, bcv_ref, dbc_ref, step_ref, run_ref, runt_ref, pay_ref,
              padx, padb):
    tokens, channels = x_ref.shape
    halo = halo_ref[...].astype(F32)
    padx[0:8, :] = halo[:, :channels]
    padb[0:8, :] = halo[:, channels:]
    padx[8:, :] = x_ref[...].astype(F32)
    padb[8:, :] = bc_ref[...].astype(F32)

    def convolved(pad, taps, bias):
        total = bias[...] + taps[0:1, :] * pad[5 : 5 + tokens, :]
        for k in range(1, 4):
            total = total + taps[k : k + 1, :] * pad[5 + k : 5 + k + tokens, :]
        sig = sigmoid(total)
        return total * sig, sig * (1.0 + total * (1.0 - sig))

    conv_bc, slope_bc = convolved(padb, cb_ref, bb_ref)
    out_high, out_low = split_two(conv_bc[:, LANES:])
    in_high, in_low = split_two(conv_bc[:, :LANES])
    bcv_ref[:, :LANES] = in_high
    bcv_ref[:, 3 * LANES :] = in_low
    bcv_ref[:, LANES : 2 * LANES] = out_high
    bcv_ref[:, 2 * LANES : 3 * LANES] = out_low
    dbc_ref[...] = slope_bc.astype(BF16)
    raw = dt_ref[...].astype(F32) + par_ref[1:2, :]
    step = softplus(raw)
    step_ref[...] = step
    decay = -step * jnp.exp(par_ref[0:1, :])
    tri = lower(CHUNK).astype(F32)
    chunks = [
        jnp.dot(tri, decay[c * CHUNK : (c + 1) * CHUNK, :], precision=HIGH, preferred_element_type=F32)
        for c in range(tokens // CHUNK)
    ]
    run = jnp.concatenate(chunks, 0)
    run_ref[...] = run
    runt_ref[...] = run.T[:16, :]
    whole, before = shard_running(run, tokens)
    heads = head_map(channels)
    weight = per_channel(jnp.exp(before[-1] - whole) * step, heads)
    conv_x, slope_x = convolved(padx, cx_ref, bx_ref)
    xv_ref[...] = conv_x.astype(BF16)
    dx_ref[...] = slope_x.astype(BF16)
    weighted = (conv_x * weight).astype(BF16)
    state = dot(in_high, weighted, 0, 0) + dot(in_low, weighted, 0, 0)
    total = jnp.broadcast_to(before[-1], (8, LANES))
    for j in range(16):
        pay_ref[j, :, :channels] = state[8 * j : 8 * j + 8, :]
        pay_ref[j, :, channels:] = total


def local_body(x_ref, bc_ref, step_ref, run_ref, runt_ref, par_ref, y_ref, sl_ref):
    tokens, channels = x_ref.shape
    heads = head_map(channels)
    run = run_ref[...]
    run_t = runt_ref[...]
    skip = per_channel(par_ref[...], heads)[2:3]
    state = None
    for c in range(tokens // CHUNK):
        rows = slice(c * CHUNK, (c + 1) * CHUNK)
        values = x_ref[rows, :].astype(F32)
        scaled = values * per_channel(step_ref[rows, :], heads)
        own_run = run[rows, :]
        last = own_run[CHUNK - 1 : CHUNK, :]
        into = bc_ref[rows, :LANES]
        out = bc_ref[rows, LANES : 2 * LANES]
        fine = bc_ref[rows, 2 * LANES : 3 * LANES]
        fine_in = bc_ref[rows, 3 * LANES :]
        scores = dot(out, into, 1, 1) + dot(fine, into, 1, 1) + dot(out, fine_in, 1, 1)
        scores = jnp.concatenate([scores, scores], 1)
        scaled16 = scaled.astype(BF16)
        result = skip * values
        if c > 0:
            sl_ref[c - 1] = state.astype(BF16)
            reads = dot(out, state.astype(BF16)) + dot(fine, state.astype(BF16))
            result = result + per_channel(jnp.exp(own_run), heads) * reads
        for pair in range(channels // LANES):
            cols = slice(pair * LANES, (pair + 1) * LANES)
            weights = (pair_weights(run, run_t, c, pair) * scores).astype(BF16)
            y_ref[rows, cols] = result[:, cols] + dot(weights, stacked(scaled16[:, cols]))
        if c < tokens // CHUNK - 1:
            to_end = per_channel(jnp.exp(last - own_run), heads)
            weighted = (to_end * scaled).astype(BF16)
            fresh = dot(into, weighted, 0, 0) + dot(fine_in, weighted, 0, 0)
            if c > 0:
                keep = per_channel(jnp.broadcast_to(jnp.exp(last), (8, LANES)), heads)[0:1]
                fresh = fresh + keep * state
            state = fresh


def shard_factors(got_ref, channels):
    totals = jnp.concatenate([got_ref[i, 0:1, channels:] for i in range(16)], 0)
    return per_channel(jnp.exp(totals), head_map(channels))


def carry_body(got_ref, out_ref):
    channels = out_ref.shape[2]
    factors = shard_factors(got_ref, channels)
    carry = jnp.zeros(out_ref.shape[1:], F32)
    for i in range(16):
        out_ref[i] = carry
        carry = factors[i : i + 1] * carry + got_ref[i, :, :channels]


def carry_back_body(got_ref, totals_ref, out_ref):
    channels = out_ref.shape[2]
    factors = shard_factors(totals_ref, channels)
    carry = jnp.zeros(out_ref.shape[1:], F32)
    for i in reversed(range(16)):
        out_ref[i] = carry.astype(BF16)
        carry = factors[i : i + 1] * carry + got_ref[i].astype(F32)


def gated_body(order_ref, y_ref, bc_ref, run_ref, s_ref, z_ref, gain_ref, do_ref, w_ref,
               mixed_ref, scaled_ref, gg_ref, sums_ref, acc):
    step = pl.program_id(0)
    tokens, channels = y_ref.shape
    product = dot(do_ref[...], w_ref[...], 0, 0)

    @pl.when(step == 0)
    def _():
        acc[...] = product
        heads = head_map(channels)
        whole, _ = shard_running(run_ref[...], tokens)
        entering, small = split_two(s_ref[...])
        out = bc_ref[:, LANES : 2 * LANES]
        reads = dot(out, entering) + dot(out, small)
        reads = reads + dot(bc_ref[:, 2 * LANES : 3 * LANES], entering)
        mixed_ref[...] = y_ref[...] + per_channel(jnp.exp(whole), heads) * reads

    @pl.when(step > 0)
    def _():
        acc[...] += product

    @pl.when(step == pl.num_programs(0) - 1)
    def _():
        gate = z_ref[...].astype(F32)
        gated = mixed_ref[...] * gate * sigmoid(gate)
        gain = gain_ref[...]
        scaled = acc[...] * gain
        scaled_ref[...] = scaled
        gg_ref[...] = (gated * gain).astype(BF16)
        squares = jnp.sum(gated * gated, axis=1, keepdims=True)
        inner = jnp.sum(gated * scaled, axis=1, keepdims=True)
        lane = lax.broadcasted_iota(jnp.int32, (tokens, LANES), 1)
        both = jnp.where(lane == 0, squares, jnp.where(lane == 1, inner, 0.0)).T[:8, :]
        for j in range(sums_ref.shape[0]):
            sums_ref[j] = both


def project_body(w_ref, gg_ref, out_ref):
    out_ref[...] = dot(w_ref[...], gg_ref[...], 1, 1).astype(BF16)


def weight_body(order_ref, do_ref, normed_ref, out_ref):
    for j in range(out_ref.shape[0]):
        size = out_ref.shape[1]
        out_ref[j] = dot(do_ref[j * size : (j + 1) * size, :], normed_ref[...]).astype(BF16)


def norm_body(sums_ref, mixed_ref, scaled_ref, z_ref, gain_ref, bc_ref, run_ref, width,
              gz_ref, gy_ref, normed_ref, pay_ref, inv_ref):
    tokens, channels = mixed_ref.shape
    heads = head_map(channels)
    total = sums_ref[0]
    for j in range(1, sums_ref.shape[0]):
        total = total + sums_ref[j]
    inv_row = lax.rsqrt(total[0:1, :] / width + EPSILON)
    inv_ref[...] = jnp.broadcast_to(inv_row, (8, tokens))
    pull_row = inv_row * inv_row * inv_row * total[1:2, :] / width
    columns = jnp.concatenate([inv_row, pull_row, jnp.zeros((LANES - 2, tokens), F32)], 0).T
    inv = columns[:, 0:1]
    pull = columns[:, 1:2]
    gate = z_ref[...].astype(F32)
    sig = sigmoid(gate)
    silu = gate * sig
    mixed = mixed_ref[...]
    gated = mixed * silu
    normed_ref[...] = (gated * inv * gain_ref[...]).astype(BF16)
    grad_gated = inv * scaled_ref[...] - gated * pull
    gz_ref[...] = grad_gated * mixed * sig * (1.0 + gate * (1.0 - sig))
    grad_mixed = grad_gated * silu
    gy_ref[...] = grad_mixed
    whole, _ = shard_running(run_ref[...], tokens)
    leading = (per_channel(jnp.exp(whole), heads) * grad_mixed).astype(BF16)
    direct = dot(bc_ref[:, LANES : 2 * LANES], leading, 0, 0)
    for j in range(16):
        pay_ref[j] = direct[8 * j : 8 * j + 8, :].astype(BF16)


def back_body(gy_ref, x_ref, bc_ref, step_ref, run_ref, runt_ref, sl_ref, s_ref,
              dxs_ref, dbc_ref, ddec_ref):
    tokens, channels = x_ref.shape
    count = tokens // CHUNK
    heads = head_map(channels)
    run = run_ref[...]
    run_t = runt_ref[...]
    before = offsets(run, tokens)
    upper = jnp.logical_not(lower(CHUNK)).astype(F32)
    reach = (lower(CHUNK).astype(F32)).T
    lane = lax.broadcasted_iota(jnp.int32, (CHUNK, LANES), 1)
    state_in = s_ref[...].astype(F32)
    flow = None
    for c in reversed(range(count)):
        rows = slice(c * CHUNK, (c + 1) * CHUNK)
        own_run = run[rows, :]
        last = own_run[CHUNK - 1 : CHUNK, :]
        into = bc_ref[rows, :LANES]
        out = bc_ref[rows, LANES : 2 * LANES]
        gy = gy_ref[rows, :]
        gy16 = gy.astype(BF16)
        scaled = x_ref[rows, :].astype(F32) * per_channel(step_ref[rows, :], heads)
        scaled16 = scaled.astype(BF16)
        small = jnp.concatenate(
            [jnp.broadcast_to(jnp.exp(before[c]), (8, LANES)), jnp.broadcast_to(jnp.exp(last), (8, LANES))], 0
        )
        small = per_channel(small, heads)
        state = small[0:1] * state_in
        if c > 0:
            state = state + sl_ref[c - 1].astype(F32)
        state16 = state.astype(BF16)
        leading = per_channel(jnp.exp(own_run), heads) * gy
        leading16 = leading.astype(BF16)
        grad_out = dot3(leading, state, 1, 1)
        reads = per_head(leading * dot(out, state16), heads)
        flat = None
        if c < count - 1:
            flow16 = flow.astype(BF16)
            to_end = per_channel(jnp.exp(last - own_run), heads)
            spread = to_end * dot(into, flow16)
            grad_in = dot3(to_end * scaled, flow, 1, 1)
            kept = per_head(scaled * spread, heads)
            flat = per_head(
                jnp.broadcast_to(jnp.sum(state * flow, axis=0, keepdims=True) * small[8:9], (8, channels)), heads
            )[0:1]
        scores = dot(out, into, 1, 1)
        scores = jnp.concatenate([scores, scores], 1)
        grad_scores = jnp.zeros((CHUNK, 2 * CHUNK), F32)
        rowsums = jnp.zeros((CHUNK, LANES), F32)
        colsums = []
        for pair in range(channels // LANES):
            cols = slice(pair * LANES, (pair + 1) * LANES)
            decays = pair_weights(run, run_t, c, pair)
            weights = decays * scores
            grad_weights = dot(gy16[:, cols], stacked(scaled16[:, cols]), 1, 1)
            grad_scores = grad_scores + grad_weights * decays
            product = grad_weights * weights
            both = dot(weights.astype(BF16), gy16[:, cols], 0, 0)
            piece = jnp.where(lanes_of(True), both[:CHUNK], both[CHUNK:])
            if c < count - 1:
                piece = piece + spread[:, cols]
            dxs_ref[rows, cols] = piece
            for side in range(2):
                half = product[:, side * CHUNK : (side + 1) * CHUNK]
                rowsums = jnp.where(lane == 2 * pair + side, jnp.sum(half, axis=1, keepdims=True), rowsums)
                colsums.append(jnp.sum(half, axis=0, keepdims=True))
        colsums = jnp.concatenate(colsums + [jnp.zeros((LANES - len(colsums), CHUNK), F32)], 0).T
        grad_scores = (grad_scores[:, :CHUNK] + grad_scores[:, CHUNK:]).astype(BF16)
        grad_out = grad_out + dot(grad_scores, into)
        own_in = dot(grad_scores, out, 0, 0)
        if c < count - 1:
            own_in = own_in + grad_in
        dbc_ref[rows, :LANES] = own_in
        dbc_ref[rows, LANES:] = grad_out
        ddec = jnp.dot(reach, rowsums - colsums + reads, precision=HIGH, preferred_element_type=F32)
        if c < count - 1:
            ddec = ddec + flat + jnp.dot(upper.T, kept, precision=HIGH, preferred_element_type=F32)
        ddec_ref[rows, :] = ddec
        if c > 0:
            fresh = dot(out, leading16, 0, 0)
            flow = fresh if flow is None else fresh + small[8:9] * flow


def final_body(a_ref, s_ref, x_ref, bc_ref, step_ref, run_ref, gy_ref, dxs_ref, dbc_ref, ddec_ref,
               dt_ref, par_ref, slx_ref, slbc_ref, cx_ref, cb_ref,
               gx_ref, gbc_ref, gdt_ref, halo_ref, padx, padb):
    tokens, channels = x_ref.shape
    heads = head_map(channels)
    whole, before = shard_running(run_ref[...], tokens)
    step = step_ref[...]
    step_wide = per_channel(step, heads)
    values = x_ref[...].astype(F32)
    scaled = values * step_wide
    after16 = a_ref[...]
    to_end = per_channel(jnp.exp(before[-1] - whole), heads)
    spread = to_end * dot(bc_ref[:, :LANES], after16)
    grad_in = dot((to_end * scaled).astype(BF16), after16, 1, 1)
    kept = per_head(scaled * spread, heads)
    total = jnp.exp(before[-1])
    cross = jnp.sum(s_ref[...].astype(F32) * after16.astype(F32), axis=0, keepdims=True)
    base = per_head(jnp.broadcast_to(cross, (8, channels)), heads)[0:1] * total
    strict = jnp.logical_not(lower(CHUNK)).astype(F32).T
    parts = []
    for c in range(tokens // CHUNK):
        own = kept[c * CHUNK : (c + 1) * CHUNK, :]
        parts.append(base + jnp.dot(strict, own, precision=HIGH, preferred_element_type=F32))
        base = base + jnp.sum(own, axis=0, keepdims=True)
    ddec = ddec_ref[...] + jnp.concatenate(parts, 0)
    dxs = dxs_ref[...] + spread
    skip = per_channel(par_ref[...], heads)[2:3]
    rate = jnp.exp(par_ref[0:1, :])
    dstep = per_head(dxs * values, heads) - ddec * rate
    gdt = dstep * sigmoid(dt_ref[...].astype(F32) + par_ref[1:2, :])
    gdt_ref[...] = gdt.T[:16, :]
    grad_conv = (dxs * step_wide + skip * gy_ref[...].astype(F32)) * slx_ref[...].astype(F32)
    padx[0:8, :] = jnp.zeros((8, channels), F32)
    padx[8 : 8 + tokens, :] = grad_conv
    padx[8 + tokens :, :] = jnp.zeros((8, channels), F32)
    padb[0:8, :] = jnp.zeros((8, 2 * LANES), F32)
    padb[8 : 8 + tokens, :LANES] = (dbc_ref[:, :LANES] + grad_in) * slbc_ref[:, :LANES].astype(F32)
    padb[8 : 8 + tokens, LANES:] = dbc_ref[:, LANES:] * slbc_ref[:, LANES:].astype(F32)
    padb[8 + tokens :, :] = jnp.zeros((8, 2 * LANES), F32)

    def transposed(pad, taps, start, size):
        result = taps[3:4, :] * pad[start : start + size, :]
        for k in range(3):
            result = result + taps[k : k + 1, :] * pad[start + 3 - k : start + 3 - k + size, :]
        return result

    gx_ref[...] = transposed(padx, cx_ref, 8, tokens)
    gbc_ref[...] = transposed(padb, cb_ref, 8, tokens)
    row = lax.broadcasted_iota(jnp.int32, (8, channels), 0)
    row_bc = lax.broadcasted_iota(jnp.int32, (8, 2 * LANES), 0)
    halo_ref[:, :channels] = jnp.where(row >= 5, transposed(padx, cx_ref, 0, 8), 0.0)
    halo_ref[:, channels:] = jnp.where(row_bc >= 5, transposed(padb, cb_ref, 0, 8), 0.0)


def call(body, outs, *args, scratch=(), grid=(), in_specs=None, out_specs=None, prefetch=0):
    scratch = [pltpu.VMEM(s, F32) for s in scratch]
    kinds = {"scratch_shapes": scratch}
    if in_specs is not None:
        kinds = {
            "grid_spec": pltpu.PrefetchScalarGridSpec(
                num_scalar_prefetch=prefetch, grid=grid, in_specs=in_specs, out_specs=out_specs,
                scratch_shapes=scratch,
            )
        }
    return pl.pallas_call(
        body,
        out_shape=[jax.ShapeDtypeStruct(s, d) for s, d in outs],
        compiler_params=pltpu.CompilerParams(vmem_limit_bytes=56 * 1024 * 1024),
        **kinds,
    )(*args)


def whole_block(shape):
    return pl.BlockSpec(shape, lambda *_: (0,) * len(shape))


def along_y(array, by, cores):
    peers = lax.axis_size("tp")
    return lax.ppermute(array, "tp", [(i, (i + by * cores) % peers) for i in range(peers)])


def from_partner(array):
    return lax.ppermute(array, "tp", [(i, i ^ 1) for i in range(lax.axis_size("tp"))])


def exchange(blocks, axis):
    return lax.all_to_all(blocks, axis, split_axis=0, concat_axis=0, tiled=True)


def shards(inner_x, gate_z, proj_bc, dt_raw, a_log, dt_bias, d_skip, conv_x, bias_x, conv_bc,
           bias_bc, norm_gain, w_out, d_out):
    tokens, channels = inner_x.shape
    n_tp = lax.axis_size("tp")
    n_seq = lax.axis_size(SEQ)
    width = float(channels * n_tp)
    tail = jnp.concatenate([inner_x[tokens - 8 :], proj_bc[tokens - 8 :]], 1)
    tail = jnp.where(jnp.arange(8)[:, None] >= 5, tail, jnp.zeros_like(tail))
    halo = lax.ppermute(tail, SEQ, [(i, i + 1) for i in range(n_seq - 1)])
    weights_t = lax.all_gather(w_out.T, SEQ, axis=0, tiled=True)
    mine = lax.axis_index("tp")
    cores = 2
    chips = n_tp // cores
    hops = (0, 1, 3, 2)
    own = d_out.T
    near = jnp.stack([own] + [along_y(own, by, cores) for by in hops[1:]])
    far = from_partner(near)
    core = mine % cores
    sources = [((mine // cores - by) % chips) * cores for by in hops]
    order = jnp.stack([y + core for y in sources] + [y + 1 - core for y in sources]).astype(jnp.int32)
    cotangent_t = jnp.concatenate([near, far]).reshape(-1, tokens)
    step_input = jnp.pad(dt_raw, ((0, 0), (0, LANES - dt_raw.shape[1])))
    params = jnp.pad(jnp.stack([a_log, dt_bias, d_skip]), ((0, 5), (0, LANES - a_log.shape[0])))
    gain = norm_gain[None, :]

    wide = (tokens, channels)
    values, slope_x, proj, slope_bc, steps, run, run_t, payload = call(
        conv_body,
        [(wide, BF16), (wide, BF16), ((tokens, 4 * LANES), BF16), (proj_bc.shape, BF16),
         ((tokens, LANES), F32), ((tokens, LANES), F32), ((16, tokens), F32), ((n_seq, 8, channels + LANES), F32)],
        inner_x, proj_bc, halo, step_input, params, conv_x, bias_x[None, :], conv_bc, bias_bc[None, :],
        scratch=[(tokens + 8, channels), (tokens + 8, 2 * LANES)],
    )
    totals = exchange(payload, SEQ)
    local, states = call(
        local_body,
        [(wide, F32), ((tokens // CHUNK - 1, LANES, channels), BF16)],
        values, proj, steps, run, run_t, params,
    )
    (entering,) = call(carry_body, [((n_seq, 8, channels), F32)], totals)
    state_in = exchange(entering, SEQ).reshape(LANES, channels)

    mixed, scaled_grad, gained, sums = call(
        gated_body,
        [(wide, F32), (wide, F32), (wide, BF16), ((n_tp, 8, tokens), F32)],
        order, local, proj, run, state_in, gate_z, gain, cotangent_t, weights_t,
        scratch=[wide], grid=(n_tp,), prefetch=1,
        in_specs=[whole_block(a.shape) for a in (local, proj, run, state_in, gate_z, gain)]
        + [pl.BlockSpec((d_out.shape[1], tokens), lambda k, order: (k, 0)),
           pl.BlockSpec((d_out.shape[1], channels), lambda k, order: (order[k], 0))],
        out_specs=[whole_block(wide)] * 3 + [whole_block((n_tp, 8, tokens))],
    )
    all_sums = exchange(sums, "tp")
    size = weights_t.shape[0] // 4
    (partial_t,) = call(
        project_body, [((weights_t.shape[0], tokens), BF16)], weights_t, gained, grid=(4,),
        in_specs=[pl.BlockSpec((size, channels), lambda k: (k, 0)), whole_block(wide)],
        out_specs=[pl.BlockSpec((size, tokens), lambda k: (k, 0))],
    )
    arrived = lax.psum_scatter(partial_t, "tp", scatter_dimension=0, tiled=True)
    grad_z, grad_mixed, normed, payload_back, inverse = call(
        lambda *refs: norm_body(*refs[:7], width, *refs[7:]),
        [(wide, F32), (wide, F32), (wide, BF16), ((n_seq, 8, channels), BF16), ((8, tokens), F32)],
        all_sums, mixed, scaled_grad, gate_z, gain, proj, run,
    )
    direct = exchange(payload_back, SEQ)

    output = (arrived.astype(F32) * inverse[0:1]).astype(BF16).T

    dxs, dproj, ddec = call(
        back_body,
        [(wide, F32), (proj_bc.shape, F32), ((tokens, LANES), F32)],
        grad_mixed, values, proj, steps, run, run_t, states, state_in,
    )
    (leaving,) = call(carry_back_body, [((n_seq, 8, channels), BF16)], direct, totals)
    after = exchange(leaving, SEQ).reshape(LANES, channels)

    part = cotangent_t.shape[0] // n_seq
    each = d_out.shape[1] // part
    (weight_t,) = call(
        weight_body, [((n_seq, part, channels), BF16)], order, cotangent_t, normed,
        grid=(n_tp,), prefetch=1,
        in_specs=[pl.BlockSpec((each * part, tokens), lambda k, order: (k, 0)), whole_block(wide)],
        out_specs=[pl.BlockSpec((each, part, channels), lambda k, order: (order[k], 0, 0))],
    )
    arrived_w = exchange(weight_t, SEQ)
    grad_w = arrived_w.astype(F32).sum(axis=0).T

    grad_x, part_bc, grad_dt, back_halo = call(
        final_body,
        [(wide, F32), (proj_bc.shape, F32), ((16, tokens), F32), ((8, channels + 2 * LANES), F32)],
        after, state_in, values, proj, steps, run, grad_mixed, dxs, dproj, ddec, step_input, params,
        slope_x, slope_bc, conv_x, conv_bc,
        scratch=[(tokens + 16, channels), (tokens + 16, 2 * LANES)],
    )
    from_next = lax.ppermute(back_halo, SEQ, [(i, i - 1) for i in range(1, n_seq)])
    grad_x = grad_x.at[tokens - 8 :].add(from_next[:, :channels])
    part_bc = part_bc.at[tokens - 8 :].add(from_next[:, channels:])
    top, bottom = part_bc[: tokens // 2], part_bc[tokens // 2 :]
    kept = jnp.where(core == 0, top, bottom)
    chip = kept + from_partner(jnp.where(core == 0, bottom, top))
    facing = chip + along_y(chip, 2, cores)
    half = facing + (along_y(chip, 1, cores) + along_y(chip, 3, cores))
    other = from_partner(half)
    grad_bc = jnp.concatenate([jnp.where(core == 0, half, other), jnp.where(core == 0, other, half)])
    grad_dt = grad_dt[: dt_raw.shape[1]].T
    return (output, grad_x, grad_z, grad_bc, grad_dt, grad_w)


def solution(mesh):
    finer = Mesh(mesh.devices.reshape(4, 4, mesh.shape["tp"]), ("seq_0", "seq_1", "tp"))
    in_specs = (
        P(SEQ, "tp"),
        P(SEQ, "tp"),
        P(SEQ, None),
        P(SEQ, "tp"),
        P("tp"),
        P("tp"),
        P("tp"),
        P(None, "tp"),
        P("tp"),
        P(),
        P(),
        P("tp"),
        P("tp", SEQ),
        P(SEQ, "tp"),
    )
    out_specs = (P(SEQ, "tp"), P(SEQ, "tp"), P(SEQ, "tp"), P(SEQ, None), P(SEQ, "tp"), P("tp", SEQ))
    return jax.shard_map(
        shards, mesh=finer, in_specs=in_specs, out_specs=out_specs, check_vma=False
    )
```

```python
import jax
import jax.numpy as jnp
from jax import lax
from jax.experimental import pallas as pl
from jax.experimental.pallas import tpu as pltpu
from jax.sharding import Mesh
from jax.sharding import PartitionSpec as P


SEQ = ("seq_0", "seq_1")
EPSILON = 1e-05
HEAD = 64
LANES = 128
CHUNK = 128
NEG = -1e30
F32 = jnp.float32
BF16 = jnp.bfloat16
HIGH = lax.Precision.HIGHEST


def dot(a, b, ca=1, cb=0):
    return lax.dot_general(a, b, (((ca,), (cb,)), ((), ())), preferred_element_type=F32)


def dot3(a, b, ca=1, cb=0):
    ah, al = split_two(a)
    bh, bl = split_two(b)
    return dot(ah, bh, ca, cb) + dot(al, bh, ca, cb) + dot(ah, bl, ca, cb)


def split_two(a):
    high = a.astype(BF16)
    return high, (a - high.astype(F32)).astype(BF16)


def head_map(channels):
    row = lax.broadcasted_iota(jnp.int32, (LANES, channels), 0)
    col = lax.broadcasted_iota(jnp.int32, (LANES, channels), 1)
    return jnp.where(lax.shift_right_logical(col, 6) == row, 1.0, 0.0).astype(BF16)


def per_channel(a, heads):
    high, low = split_two(a)
    return dot(high, heads) + dot(low, heads)


def per_head(a, heads):
    high, low = split_two(a)
    return dot(high, heads, 1, 1) + dot(low, heads, 1, 1)


def sigmoid(v):
    return 1.0 / (1.0 + jnp.exp(-v))


def softplus(v):
    return jnp.maximum(v, 0.0) + jnp.log1p(jnp.exp(-jnp.abs(v)))


def lower(size):
    return lax.broadcasted_iota(jnp.int32, (size, size), 0) >= lax.broadcasted_iota(
        jnp.int32, (size, size), 1
    )


def offsets(run, tokens):
    before = [jnp.zeros((1, LANES), F32)]
    for c in range(tokens // CHUNK):
        before.append(before[-1] + run[(c + 1) * CHUNK - 1 : (c + 1) * CHUNK, :])
    return before


def shard_running(run, tokens):
    before = offsets(run, tokens)
    parts = [run[c * CHUNK : (c + 1) * CHUNK, :] + before[c] for c in range(tokens // CHUNK)]
    return jnp.concatenate(parts, 0), before


def lanes_of(first):
    lane = lax.broadcasted_iota(jnp.int32, (CHUNK, LANES), 1)
    return lane < HEAD if first else lane >= HEAD


def stacked(block):
    zero = jnp.zeros_like(block)
    return jnp.concatenate(
        [jnp.where(lanes_of(True), block, zero), jnp.where(lanes_of(False), block, zero)], 0
    )


def pair_weights(run, run_t, pair):
    sides = []
    for h in (2 * pair, 2 * pair + 1):
        spread = run[:, h : h + 1] - run_t[h : h + 1, :]
        sides.append(jnp.exp(jnp.where(lower(CHUNK), spread, NEG)))
    return jnp.concatenate(sides, 1)


def conv_body(x_ref, bc_ref, halo_ref, dt_ref, par_ref, cx_ref, bx_ref, cb_ref, bb_ref,
              xv_ref, dx_ref, bcv_ref, dbc_ref, step_ref, run_ref, runt_ref, before_ref, pay_ref,
              padx, padb):
    tokens, channels = x_ref.shape
    halo = halo_ref[...].astype(F32)
    padx[0:8, :] = halo[:, :channels]
    padb[0:8, :] = halo[:, channels:]
    padx[8:, :] = x_ref[...].astype(F32)
    padb[8:, :] = bc_ref[...].astype(F32)

    def convolved(pad, taps, bias):
        total = bias[...] + taps[0:1, :] * pad[5 : 5 + tokens, :]
        for k in range(1, 4):
            total = total + taps[k : k + 1, :] * pad[5 + k : 5 + k + tokens, :]
        sig = sigmoid(total)
        return total * sig, sig * (1.0 + total * (1.0 - sig))

    conv_bc, slope_bc = convolved(padb, cb_ref, bb_ref)
    out_high, out_low = split_two(conv_bc[:, LANES:])
    in_high, in_low = split_two(conv_bc[:, :LANES])
    bcv_ref[:, :LANES] = in_high
    bcv_ref[:, 3 * LANES :] = in_low
    bcv_ref[:, LANES : 2 * LANES] = out_high
    bcv_ref[:, 2 * LANES : 3 * LANES] = out_low
    dbc_ref[...] = slope_bc.astype(BF16)
    raw = dt_ref[...].astype(F32) + par_ref[1:2, :]
    step = softplus(raw)
    step_ref[...] = step
    decay = -step * jnp.exp(par_ref[0:1, :])
    tri = lower(CHUNK).astype(F32)
    chunks = [
        jnp.dot(tri, decay[c * CHUNK : (c + 1) * CHUNK, :], precision=HIGH, preferred_element_type=F32)
        for c in range(tokens // CHUNK)
    ]
    run = jnp.concatenate(chunks, 0)
    run_ref[...] = run
    runt_ref[...] = run.T[:16, :]
    whole, before = shard_running(run, tokens)
    before_ref[...] = jnp.concatenate(before + [jnp.zeros((8 - len(before), LANES), F32)], 0)
    heads = head_map(channels)
    weight = per_channel(jnp.exp(before[-1] - whole) * step, heads)
    conv_x, slope_x = convolved(padx, cx_ref, bx_ref)
    xv_ref[...] = conv_x.astype(BF16)
    dx_ref[...] = slope_x.astype(BF16)
    weighted = (conv_x * weight).astype(BF16)
    state = dot(in_high, weighted, 0, 0) + dot(in_low, weighted, 0, 0)
    total = jnp.broadcast_to(before[-1], (8, LANES))
    for j in range(16):
        pay_ref[j, :, :channels] = state[8 * j : 8 * j + 8, :]
        pay_ref[j, :, channels:] = total


def local_body(x_ref, bc_ref, step_ref, run_ref, runt_ref, par_ref, y_ref, sl_ref, state_ref):
    @pl.when(pl.program_id(0) == 0)
    def _():
        state_ref[...] = jnp.zeros_like(state_ref)

    channels = x_ref.shape[1]
    heads = head_map(channels)
    run = run_ref[...]
    run_t = runt_ref[...]
    skip = per_channel(par_ref[...], heads)[2:3]
    values = x_ref[...].astype(F32)
    scaled = values * per_channel(step_ref[...], heads)
    last = run[CHUNK - 1 : CHUNK, :]
    into = bc_ref[:, :LANES]
    out = bc_ref[:, LANES : 2 * LANES]
    fine = bc_ref[:, 2 * LANES : 3 * LANES]
    fine_in = bc_ref[:, 3 * LANES :]
    scores = dot(out, into, 1, 1) + dot(fine, into, 1, 1) + dot(out, fine_in, 1, 1)
    scores = jnp.concatenate([scores, scores], 1)
    scaled16 = scaled.astype(BF16)
    state = state_ref[...]
    state16 = state.astype(BF16)
    sl_ref[0] = state16
    reads = dot(out, state16) + dot(fine, state16)
    result = skip * values + per_channel(jnp.exp(run), heads) * reads
    for pair in range(channels // LANES):
        cols = slice(pair * LANES, (pair + 1) * LANES)
        weights = (pair_weights(run, run_t, pair) * scores).astype(BF16)
        y_ref[:, cols] = result[:, cols] + dot(weights, stacked(scaled16[:, cols]))
    to_end = per_channel(jnp.exp(last - run), heads)
    weighted = (to_end * scaled).astype(BF16)
    keep = per_channel(jnp.broadcast_to(jnp.exp(last), (8, LANES)), heads)[0:1]
    state_ref[...] = keep * state + dot(into, weighted, 0, 0) + dot(fine_in, weighted, 0, 0)


def shard_factors(got_ref, channels):
    totals = jnp.concatenate([got_ref[i, 0:1, channels:] for i in range(16)], 0)
    return per_channel(jnp.exp(totals), head_map(channels))


def carry_body(got_ref, out_ref):
    channels = out_ref.shape[2]
    factors = shard_factors(got_ref, channels)
    carry = jnp.zeros(out_ref.shape[1:], F32)
    for i in range(16):
        out_ref[i] = carry
        carry = factors[i : i + 1] * carry + got_ref[i, :, :channels]


def carry_back_body(got_ref, totals_ref, out_ref):
    channels = out_ref.shape[2]
    factors = shard_factors(totals_ref, channels)
    carry = jnp.zeros(out_ref.shape[1:], F32)
    for i in reversed(range(16)):
        out_ref[i] = carry.astype(BF16)
        carry = factors[i : i + 1] * carry + got_ref[i].astype(F32)


def gated_body(s_ref, order_ref, y_ref, bc_ref, run_ref, z_ref, gain_ref, near_ref, far_ref, w_ref,
               mixed_ref, gn_ref, gg_ref, sums_ref):
    tokens, channels = y_ref.shape
    heads = head_map(channels)
    whole, _ = shard_running(run_ref[...], tokens)
    entering, small = split_two(s_ref[...])
    out = bc_ref[:, LANES : 2 * LANES]
    reads = dot(out, entering) + dot(out, small)
    reads = reads + dot(bc_ref[:, 2 * LANES : 3 * LANES], entering)
    mixed = y_ref[...] + per_channel(jnp.exp(whole), heads) * reads
    mixed_ref[...] = mixed
    gate = z_ref[...].astype(F32)
    gained = mixed * gate * sigmoid(gate)
    squares = jnp.sum(gained * gained, axis=1, keepdims=True)
    gained = gained * gain_ref[...]
    gg_ref[...] = gained.astype(BF16)
    count, size = near_ref.shape[0], near_ref.shape[1]
    left = [near_ref[i] for i in range(count)] + [far_ref[i] for i in range(count)]
    right = [w_ref[pl.ds(pl.multiple_of(order_ref[i] * size, 64), size), :] for i in range(2 * count)]
    grad = dot(jnp.concatenate(left, 0), jnp.concatenate(right, 0), 0, 0)
    gn_ref[...] = grad
    inner = jnp.sum(gained * grad, axis=1, keepdims=True)
    lane = lax.broadcasted_iota(jnp.int32, (tokens, LANES), 1)
    both = jnp.where(lane == 0, squares, jnp.where(lane == 1, inner, 0.0)).T[:8, :]
    for j in range(sums_ref.shape[0]):
        sums_ref[j] = both


def project_body(w_ref, gg_ref, out_ref):
    out_ref[...] = dot(w_ref[...], gg_ref[...], 1, 1).astype(BF16)


def weight_body(order_ref, near_ref, far_ref, normed_ref, out_ref):
    core = order_ref[0] & 1
    part = out_ref.shape[1]
    normed = normed_ref[...]
    for source, base in ((near_ref, 2 * core), (far_ref, 2 - 2 * core)):
        block = dot(source[0], normed).astype(BF16)
        out_ref[base] = block[:part]
        out_ref[base + 1] = block[part:]


def token_columns(first, second):
    tokens = first.shape[1]
    columns = jnp.concatenate([first, second, jnp.zeros((LANES - 2, tokens), F32)], 0).T
    return columns[:, 0:1], columns[:, 1:2]


def gate_body(scale_ref, mixed_ref, gn_ref, z_ref, gain_ref, gz_ref):
    inv, pull = token_columns(scale_ref[0:1, :], scale_ref[1:2, :])
    gate = z_ref[...].astype(F32)
    sig = sigmoid(gate)
    mixed = mixed_ref[...]
    grad_gated = inv * (gn_ref[...] * gain_ref[...]) - mixed * gate * sig * pull
    gz_ref[...] = grad_gated * mixed * sig * (1.0 + gate * (1.0 - sig))


def norm_body(sums_ref, mixed_ref, scaled_ref, z_ref, gain_ref, bc_ref, run_ref, width,
              gy_ref, normed_ref, pay_ref, inv_ref):
    tokens, channels = mixed_ref.shape
    heads = head_map(channels)
    total = sums_ref[0]
    for j in range(1, sums_ref.shape[0]):
        total = total + sums_ref[j]
    inv_row = lax.rsqrt(total[0:1, :] / width + EPSILON)
    pull_row = inv_row * inv_row * inv_row * total[1:2, :] / width
    index = lax.broadcasted_iota(jnp.int32, (8, tokens), 0)
    inv_ref[...] = jnp.where(index == 0, inv_row, pull_row)
    inv, pull = token_columns(inv_row, pull_row)
    gate = z_ref[...].astype(F32)
    sig = sigmoid(gate)
    silu = gate * sig
    mixed = mixed_ref[...]
    gated = mixed * silu
    normed_ref[...] = (gated * inv * gain_ref[...]).astype(BF16)
    grad_gated = inv * (scaled_ref[...] * gain_ref[...]) - gated * pull
    grad_mixed = grad_gated * silu
    gy_ref[...] = grad_mixed
    whole, _ = shard_running(run_ref[...], tokens)
    leading = (per_channel(jnp.exp(whole), heads) * grad_mixed).astype(BF16)
    direct = dot(bc_ref[:, LANES : 2 * LANES], leading, 0, 0)
    for j in range(16):
        pay_ref[j] = direct[8 * j : 8 * j + 8, :].astype(BF16)


def back_body(gy_ref, x_ref, bc_ref, step_ref, run_ref, runt_ref, sl_ref, s_ref, before_ref,
              dxs_ref, dbc_ref, ddec_ref, flow_ref):
    @pl.when(pl.program_id(0) == 0)
    def _():
        flow_ref[...] = jnp.zeros_like(flow_ref)

    chunk = pl.num_programs(0) - 1 - pl.program_id(0)
    channels = x_ref.shape[1]
    heads = head_map(channels)
    run = run_ref[...]
    run_t = runt_ref[...]
    reach = (lower(CHUNK).astype(F32)).T
    behind = jnp.logical_not(lower(CHUNK)).astype(F32).T
    lane = lax.broadcasted_iota(jnp.int32, (CHUNK, LANES), 1)
    last = run[CHUNK - 1 : CHUNK, :]
    into = bc_ref[:, :LANES]
    out = bc_ref[:, LANES : 2 * LANES]
    gy = gy_ref[...]
    gy16 = gy.astype(BF16)
    scaled = x_ref[...].astype(F32) * per_channel(step_ref[...], heads)
    scaled16 = scaled.astype(BF16)
    ahead = before_ref[pl.ds(chunk, 1), :]
    small = jnp.concatenate(
        [jnp.broadcast_to(jnp.exp(ahead), (8, LANES)), jnp.broadcast_to(jnp.exp(last), (8, LANES))], 0
    )
    small = per_channel(small, heads)
    state = small[0:1] * s_ref[...].astype(F32) + sl_ref[0].astype(F32)
    flow = flow_ref[...]
    flow16 = flow.astype(BF16)
    leading = per_channel(jnp.exp(run), heads) * gy
    leading16 = leading.astype(BF16)
    grad_out = dot3(leading, state, 1, 1)
    reads = per_head(leading * dot(out, state.astype(BF16)), heads)
    to_end = per_channel(jnp.exp(last - run), heads)
    spread = to_end * dot(into, flow16)
    grad_in = dot3(to_end * scaled, flow, 1, 1)
    kept = per_head(scaled * spread, heads)
    flat = per_head(
        jnp.broadcast_to(jnp.sum(state * flow, axis=0, keepdims=True) * small[8:9], (8, channels)), heads
    )[0:1]
    scores = dot(out, into, 1, 1)
    scores = jnp.concatenate([scores, scores], 1)
    grad_scores = jnp.zeros((CHUNK, 2 * CHUNK), F32)
    rowsums = jnp.zeros((CHUNK, LANES), F32)
    colsums = []
    for pair in range(channels // LANES):
        cols = slice(pair * LANES, (pair + 1) * LANES)
        decays = pair_weights(run, run_t, pair)
        weights = decays * scores
        grad_weights = dot(gy16[:, cols], stacked(scaled16[:, cols]), 1, 1)
        grad_scores = grad_scores + grad_weights * decays
        product = grad_weights * weights
        both = dot(weights.astype(BF16), gy16[:, cols], 0, 0)
        dxs_ref[:, cols] = jnp.where(lanes_of(True), both[:CHUNK], both[CHUNK:]) + spread[:, cols]
        for side in range(2):
            half = product[:, side * CHUNK : (side + 1) * CHUNK]
            rowsums = jnp.where(lane == 2 * pair + side, jnp.sum(half, axis=1, keepdims=True), rowsums)
            colsums.append(jnp.sum(half, axis=0, keepdims=True))
    colsums = jnp.concatenate(colsums + [jnp.zeros((LANES - len(colsums), CHUNK), F32)], 0).T
    grad_scores = (grad_scores[:, :CHUNK] + grad_scores[:, CHUNK:]).astype(BF16)
    dbc_ref[:, :LANES] = dot(grad_scores, out, 0, 0) + grad_in
    dbc_ref[:, LANES:] = grad_out + dot(grad_scores, into)
    ddec = jnp.dot(reach, rowsums - colsums + reads, precision=HIGH, preferred_element_type=F32)
    ddec_ref[...] = ddec + flat + jnp.dot(behind, kept, precision=HIGH, preferred_element_type=F32)
    flow_ref[...] = small[8:9] * flow + dot(out, leading16, 0, 0)


def transposed(pad, taps, start, size):
    result = taps[3:4, :] * pad[start : start + size, :]
    for k in range(3):
        result = result + taps[k : k + 1, :] * pad[start + 3 - k : start + 3 - k + size, :]
    return result


def ends_body(a_ref, x_ref, bc_ref, step_ref, run_ref, gy_ref, dxs_ref, dbc_ref, par_ref,
              slx_ref, slbc_ref, cx_ref, cb_ref, gbc_ref, halo_ref, kept_ref, padx, padb):
    tokens, channels = x_ref.shape
    heads = head_map(channels)
    whole, before = shard_running(run_ref[...], tokens)
    step_wide = per_channel(step_ref[...], heads)
    to_end = per_channel(jnp.exp(before[-1] - whole), heads)
    ending = (to_end * (x_ref[...].astype(F32) * step_wide)).astype(BF16)
    after16 = a_ref[...]
    grad_in = dot(ending, after16, 1, 1)
    kept_ref[...] = per_head(ending.astype(F32) * dot(bc_ref[:, :LANES], after16), heads)
    padb[0:8, :] = jnp.zeros((8, 2 * LANES), F32)
    padb[8 : 8 + tokens, :LANES] = (dbc_ref[:, :LANES] + grad_in) * slbc_ref[:, :LANES].astype(F32)
    padb[8 : 8 + tokens, LANES:] = dbc_ref[:, LANES:] * slbc_ref[:, LANES:].astype(F32)
    padb[8 + tokens :, :] = jnp.zeros((8, 2 * LANES), F32)
    gbc_ref[0:tokens, :] = transposed(padb, cb_ref, 8, tokens)
    row_bc = lax.broadcasted_iota(jnp.int32, (8, 2 * LANES), 0)
    gbc_ref[tokens : tokens + 8, :] = jnp.where(row_bc >= 5, transposed(padb, cb_ref, 0, 8), 0.0)
    gbc_ref[tokens + 8 :, :] = jnp.zeros((8, 2 * LANES), F32)
    first = slice(0, 16)
    skip = per_channel(par_ref[...], heads)[2:3]
    dxs = dxs_ref[first, :] + to_end[first] * dot(bc_ref[first, :LANES], after16)
    grad_conv = (dxs * step_wide[first] + skip * gy_ref[first, :].astype(F32)) * slx_ref[first, :].astype(F32)
    padx[0:8, :] = jnp.zeros((8, channels), F32)
    padx[8:24, :] = grad_conv
    row = lax.broadcasted_iota(jnp.int32, (8, channels), 0)
    halo_ref[...] = jnp.where(row >= 5, transposed(padx, cx_ref, 0, 8), 0.0)


def final_body(a_ref, s_ref, x_ref, bc_ref, step_ref, run_ref, gy_ref, dxs_ref, ddec_ref, kept_ref,
               dt_ref, par_ref, slx_ref, cx_ref, gx_ref, gdt_ref, padx):
    tokens, channels = x_ref.shape
    heads = head_map(channels)
    whole, before = shard_running(run_ref[...], tokens)
    step_wide = per_channel(step_ref[...], heads)
    after16 = a_ref[...]
    to_end = per_channel(jnp.exp(before[-1] - whole), heads)
    dxs = dxs_ref[...] + to_end * dot(bc_ref[:, :LANES], after16)
    skip = per_channel(par_ref[...], heads)[2:3]
    padx[0:tokens, :] = (dxs * step_wide + skip * gy_ref[...].astype(F32)) * slx_ref[...].astype(F32)
    padx[tokens:, :] = jnp.zeros((8, channels), F32)
    gx_ref[...] = transposed(padx, cx_ref, 0, tokens)
    kept = kept_ref[...]
    cross = jnp.sum(s_ref[...].astype(F32) * after16.astype(F32), axis=0, keepdims=True)
    base = per_head(jnp.broadcast_to(cross, (8, channels)), heads)[0:1] * jnp.exp(before[-1])
    strict = jnp.logical_not(lower(CHUNK)).astype(F32).T
    parts = []
    for c in range(tokens // CHUNK):
        own = kept[c * CHUNK : (c + 1) * CHUNK, :]
        parts.append(base + jnp.dot(strict, own, precision=HIGH, preferred_element_type=F32))
        base = base + jnp.sum(own, axis=0, keepdims=True)
    ddec = ddec_ref[...] + jnp.concatenate(parts, 0)
    rate = jnp.exp(par_ref[0:1, :])
    dstep = per_head(dxs * x_ref[...].astype(F32), heads) - ddec * rate
    gdt = dstep * sigmoid(dt_ref[...].astype(F32) + par_ref[1:2, :])
    gdt_ref[...] = gdt.T[:16, :]


def call(body, outs, *args, scratch=(), grid=(), in_specs=None, out_specs=None, prefetch=0,
         at_hand=(0,), scalars=(), room=56):
    scratch = [pltpu.VMEM(s, F32) for s in scratch]
    if in_specs is None:
        in_specs = [
            pl.BlockSpec(memory_space=pltpu.SMEM if i in scalars else pltpu.VMEM if i in at_hand else None)
            for i in range(len(args))
        ]
        kinds = {"scratch_shapes": scratch, "in_specs": in_specs}
    else:
        kinds = {
            "grid_spec": pltpu.PrefetchScalarGridSpec(
                num_scalar_prefetch=prefetch, grid=grid, in_specs=in_specs, out_specs=out_specs,
                scratch_shapes=scratch,
            )
        }
    return pl.pallas_call(
        body,
        out_shape=[jax.ShapeDtypeStruct(s, d) for s, d in outs],
        compiler_params=pltpu.CompilerParams(vmem_limit_bytes=room * 1024 * 1024),
        **kinds,
    )(*args)


def whole_block(shape):
    return pl.BlockSpec(shape, lambda *_: (0,) * len(shape))


def along_y(array, by, cores):
    peers = lax.axis_size("tp")
    return lax.ppermute(array, "tp", [(i, (i + by * cores) % peers) for i in range(peers)])


def from_partner(array):
    return lax.ppermute(array, "tp", [(i, i ^ 1) for i in range(lax.axis_size("tp"))])


def exchange(blocks, axis):
    return lax.all_to_all(blocks, axis, split_axis=0, concat_axis=0, tiled=True)


def shards(inner_x, gate_z, proj_bc, dt_raw, a_log, dt_bias, d_skip, conv_x, bias_x, conv_bc,
           bias_bc, norm_gain, w_out, d_out):
    tokens, channels = inner_x.shape
    n_tp = lax.axis_size("tp")
    n_seq = lax.axis_size(SEQ)
    width = float(channels * n_tp)
    tail = jnp.concatenate([inner_x[tokens - 8 :], proj_bc[tokens - 8 :]], 1)
    tail = jnp.where(jnp.arange(8)[:, None] >= 5, tail, jnp.zeros_like(tail))
    halo = lax.ppermute(tail, SEQ, [(i, i + 1) for i in range(n_seq - 1)])
    weights_t = lax.all_gather(w_out.T, SEQ, axis=0, tiled=True)
    mine = lax.axis_index("tp")
    cores = 2
    chips = n_tp // cores
    hops = (0, 1, 3, 2)
    own = d_out.T
    near = jnp.stack([own] + [along_y(own, by, cores) for by in hops[1:]])
    far = from_partner(near)
    core = mine % cores
    sources = [((mine // cores - by) % chips) * cores for by in hops]
    order = jnp.stack([y + core for y in sources] + [y + 1 - core for y in sources]).astype(jnp.int32)
    step_input = jnp.pad(dt_raw, ((0, 0), (0, LANES - dt_raw.shape[1])))
    params = jnp.pad(jnp.stack([a_log, dt_bias, d_skip]), ((0, 5), (0, LANES - a_log.shape[0])))
    gain = norm_gain[None, :]

    wide = (tokens, channels)
    values, slope_x, proj, slope_bc, steps, run, run_t, ahead, payload = call(
        conv_body,
        [(wide, BF16), (wide, BF16), ((tokens, 4 * LANES), BF16), (proj_bc.shape, BF16),
         ((tokens, LANES), F32), ((tokens, LANES), F32), ((16, tokens), F32), ((8, LANES), F32),
         ((n_seq, 8, channels + LANES), F32)],
        inner_x, proj_bc, halo, step_input, params, conv_x, bias_x[None, :], conv_bc, bias_bc[None, :], at_hand=(2,),
        scratch=[(tokens + 8, channels), (tokens + 8, 2 * LANES)],
    )
    totals = exchange(payload, SEQ)
    count = tokens // CHUNK

    def chunked(last, place):
        return pl.BlockSpec((CHUNK, last), lambda k: (place(k), 0))

    forward = lambda k: k
    local, states = call(
        local_body, [(wide, F32), ((count, LANES, channels), BF16)],
        values, proj, steps, run, run_t, params,
        grid=(count,), scratch=[(LANES, channels)],
        in_specs=[chunked(a.shape[1], forward) for a in (values, proj, steps, run)]
        + [pl.BlockSpec((16, CHUNK), lambda k: (0, k)), whole_block(params.shape)],
        out_specs=[chunked(channels, forward), pl.BlockSpec((1, LANES, channels), lambda k: (k, 0, 0))],
    )
    (entering,) = call(carry_body, [((n_seq, 8, channels), F32)], totals)
    state_in = exchange(entering, SEQ).reshape(LANES, channels)

    piece = d_out.shape[1]
    mixed, grad_normed, gained, sums = call(
        gated_body, [(wide, F32), (wide, F32), (wide, BF16), ((n_tp, 8, tokens), F32)],
        state_in, order, local, proj, run, gate_z, gain, near, far, weights_t, scalars=(1,),
    )
    all_sums = exchange(sums, "tp")
    size = weights_t.shape[0] // 4
    (partial_t,) = call(
        project_body, [((weights_t.shape[0], tokens), BF16)], weights_t, gained, grid=(4,),
        in_specs=[pl.BlockSpec((size, channels), lambda k: (k, 0)), whole_block(wide)],
        out_specs=[pl.BlockSpec((size, tokens), lambda k: (k, 0))],
    )
    arrived = lax.psum_scatter(partial_t, "tp", scatter_dimension=0, tiled=True)
    grad_mixed, normed, payload_back, inverse = call(
        lambda *refs: norm_body(*refs[:7], width, *refs[7:]),
        [(wide, F32), (wide, BF16), ((n_seq, 8, channels), BF16), ((8, tokens), F32)],
        all_sums, mixed, grad_normed, gate_z, gain, proj, run,
    )
    direct = exchange(payload_back, SEQ)
    (grad_z,) = call(gate_body, [(wide, F32)], inverse, mixed, grad_normed, gate_z, gain, at_hand=())

    output = (arrived.astype(F32) * inverse[0:1]).astype(BF16).T

    backward = lambda k: count - 1 - k
    dxs, dproj, ddec = call(
        back_body, [(wide, F32), (proj_bc.shape, F32), ((tokens, LANES), F32)],
        grad_mixed, values, proj, steps, run, run_t, states, state_in, ahead,
        grid=(count,), scratch=[(LANES, channels)],
        in_specs=[chunked(a.shape[1], backward) for a in (grad_mixed, values, proj, steps, run)]
        + [pl.BlockSpec((16, CHUNK), lambda k: (0, backward(k))),
           pl.BlockSpec((1, LANES, channels), lambda k: (backward(k), 0, 0)),
           whole_block(state_in.shape), whole_block(ahead.shape)],
        out_specs=[chunked(a, backward) for a in (channels, 2 * LANES, LANES)],
    )
    (leaving,) = call(carry_back_body, [((n_seq, 8, channels), BF16)], direct, totals)
    after = exchange(leaving, SEQ).reshape(LANES, channels)

    part = weights_t.shape[0] // n_seq
    each = n_seq // chips
    (weight_t,) = call(
        weight_body, [((n_seq, part, channels), BF16)], order, near, far, normed,
        grid=(chips,), prefetch=1,
        in_specs=[pl.BlockSpec((1, piece, tokens), lambda k, order: (k, 0, 0))] * 2 + [whole_block(wide)],
        out_specs=[pl.BlockSpec((each, part, channels), lambda k, order: (order[k] >> 1, 0, 0))],
    )
    arrived_w = exchange(weight_t, SEQ)
    grad_w = arrived_w.astype(F32).sum(axis=0).T

    part_bc, back_halo, kept_sums = call(
        ends_body, [((tokens + 16, 2 * LANES), F32), ((8, channels), F32), ((tokens, LANES), F32)],
        after, values, proj, steps, run, grad_mixed, dxs, dproj, params, slope_x, slope_bc, conv_x, conv_bc,
        scratch=[(24, channels), (tokens + 16, 2 * LANES)],
    )
    grad_x, grad_dt = call(
        final_body, [(wide, F32), ((16, tokens), F32)],
        after, state_in, values, proj, steps, run, grad_mixed, dxs, ddec, kept_sums, step_input, params,
        slope_x, conv_x,
        scratch=[(tokens + 8, channels)],
    )
    middle = part_bc.shape[0] // 2
    top, bottom = part_bc[:middle], part_bc[middle:]
    kept = jnp.where(core == 0, top, bottom)
    chip = kept + from_partner(jnp.where(core == 0, bottom, top))
    facing = chip + along_y(chip, 2, cores)
    half = facing + (along_y(chip, 1, cores) + along_y(chip, 3, cores))
    other = from_partner(half)
    summed = jnp.concatenate([jnp.where(core == 0, half, other), jnp.where(core == 0, other, half)])
    edge = jnp.concatenate([back_halo, summed[tokens : tokens + 8]], 1)
    from_next = lax.ppermute(edge, SEQ, [(i, i - 1) for i in range(1, n_seq)])
    grad_x = grad_x.at[tokens - 8 :].add(from_next[:, :channels])
    grad_bc = summed[:tokens].at[tokens - 8 :].add(from_next[:, channels:])
    grad_dt = grad_dt[: dt_raw.shape[1]].T
    return (output, grad_x, grad_z, grad_bc, grad_dt, grad_w)


def solution(mesh):
    finer = Mesh(mesh.devices.reshape(4, 4, mesh.shape["tp"]), ("seq_0", "seq_1", "tp"))
    in_specs = (
        P(SEQ, "tp"),
        P(SEQ, "tp"),
        P(SEQ, None),
        P(SEQ, "tp"),
        P("tp"),
        P("tp"),
        P("tp"),
        P(None, "tp"),
        P("tp"),
        P(),
        P(),
        P("tp"),
        P("tp", SEQ),
        P(SEQ, "tp"),
    )
    out_specs = (P(SEQ, "tp"), P(SEQ, "tp"), P(SEQ, "tp"), P(SEQ, None), P(SEQ, "tp"), P("tp", SEQ))
    return jax.shard_map(shards, mesh=finer, in_specs=in_specs, out_specs=out_specs, check_vma=False)
```
